32 devices in a mesh: gx: 4 (over z), gy: 4 (over y, x), gz: 2 (over core).
Axes of the slice: x: 2, y: 2, z: 4, core: 2. Of those that a mesh axis runs over, the one named last changes fastest.
Arguments:
- potential: float32 [16, 96, 512], P('gz', 'gx', 'gy'), may hold values from -6 to 6
- tissue_mask: int32 [16, 96, 512], P('gz', 'gx', 'gy'), may hold values from 0 to 2, as said below
- layer_index: int32 [16], P('gz'), may hold values from 0 to 15
- source: float32 [16, 96, 512], P('gz', 'gx', 'gy'), may hold values from -6 to 6
Outputs:
- phi_e: float32 [16, 96, 512], P('gz', 'gx', 'gy')
- residual: float32 [16, 96, 512], P('gz', 'gx', 'gy')
The draws below stay inside these ranges and needn't reach their ends.
Inputs may be any that keep to these rules, and one draw needn't show every extreme that they name: `tissue_mask`: 0 marks cells outside every medium, 1 bath, 2 tissue.
All inputs are finite; a program needn't handle non-finite values.
Results may differ from the reference program's by a relative error of at most 0.0003.
Values sent between devices are 32-bit elements; how exact they have to be, the bound alone decides.
A program may use at most 128 MiB of HBM per device.

```python
import math
import jax
import jax.numpy as jnp

ITERS = 8
LAYERS = 16
NZ = 16
NX = 96
NY = 512


def cell_axes():
    plane_z = jnp.arange(NZ, dtype=jnp.float32)[:, None, None] + 0.5
    row_x = jnp.arange(NX, dtype=jnp.float32)[None, :, None] + 0.5
    column_y = jnp.arange(NY, dtype=jnp.float32)[None, None, :] + 0.5
    return (plane_z, row_x, column_y)


def draw_tissue_mask(key, part):
    centre_key = jax.random.fold_in(key, 101)
    radius_key = jax.random.fold_in(key, 103)
    jitter_key = jax.random.fold_in(key, 107)
    shift = jax.random.randint(centre_key, (3,), -8, 9)
    centre_z = NZ // 2 + shift[0] * NZ // 64
    centre_x = NX // 2 + shift[1] * NX // 64
    centre_y = NY // 2 + shift[2] * NY // 64
    plane_z = jnp.arange(NZ, dtype=jnp.int32)[:, None, None]
    row_x = jnp.arange(NX, dtype=jnp.int32)[None, :, None]
    column_y = jnp.arange(NY, dtype=jnp.int32)[None, None, :]
    scaled_z = 128 * (plane_z - centre_z) // NZ
    scaled_x = 128 * (row_x - centre_x) // NX
    scaled_y = 128 * (column_y - centre_y) // NY
    reach = scaled_z * scaled_z + scaled_x * scaled_x + scaled_y * scaled_y
    reach = reach + jax.random.randint(jitter_key, (NZ, NX, NY), -150, 151)
    inner_key, outer_key, bath_key = jax.random.split(radius_key, 3)
    inner_edge = jax.random.randint(inner_key, (), 600, 1001)
    outer_edge = jax.random.randint(outer_key, (), 1900, 2501)
    bath_edge = jax.random.randint(bath_key, (), 3200, 4201)
    labels = jnp.where(reach < inner_edge, 1, jnp.where(reach < outer_edge, 2, jnp.where(reach < bath_edge, 1, 0)))
    return labels.astype(jnp.int32)


def draw_potential(key, part):
    normal_key = jax.random.fold_in(key, 201)
    anchor_key = jax.random.fold_in(key, 203)
    shape_key = jax.random.fold_in(key, 207)
    noise_key = jax.random.fold_in(key, 211)
    plane_z, row_x, column_y = cell_axes()
    sizes = jnp.array([NZ, NX, NY], jnp.float32)
    anchor = jax.random.uniform(anchor_key, (3,), jnp.float32, 0.3, 0.7) * sizes
    amp_key, width_key = jax.random.split(shape_key, 2)
    width = jax.random.uniform(width_key, (), jnp.float32, 2.0, 5.0)
    direction = jax.random.normal(normal_key, (3,), jnp.float32)
    direction = direction / jnp.sqrt(jnp.sum(direction * direction) + 1e-06)
    signed = direction[0] * (plane_z - anchor[0]) + direction[1] * (row_x - anchor[1]) + direction[2] * (column_y - anchor[2])
    amplitude = jax.random.uniform(amp_key, (), jnp.float32, 2.0, 4.0)
    noise = jnp.clip(0.5 * jax.random.normal(noise_key, (NZ, NX, NY), jnp.float32), -2.0, 2.0)
    return (amplitude * jnp.tanh(signed / width) + noise).astype(jnp.float32)


def draw_source(key, part):
    sign_key = jax.random.fold_in(key, 301)
    level_key = jax.random.fold_in(key, 303)
    mode_key = jax.random.fold_in(key, 307)
    weight_key = jax.random.fold_in(key, 311)
    noise_key = jax.random.fold_in(key, 313)
    plane_z, row_x, column_y = cell_axes()
    sign = jnp.where(jax.random.bernoulli(sign_key), 1.0, -1.0).astype(jnp.float32)
    orders = jax.random.randint(mode_key, (3, 3), 0, 3).astype(jnp.float32)
    level = jax.random.uniform(level_key, (), jnp.float32, 0.5, 1.0)
    weights = jax.random.uniform(weight_key, (3,), jnp.float32, -0.5, 0.5)
    noise = jnp.clip(jax.random.normal(noise_key, (NZ, NX, NY), jnp.float32), -3.0, 3.0)
    smooth = jnp.zeros((NZ, NX, NY), jnp.float32)
    for mode in range(3):
        wave = jnp.cos(math.pi * orders[mode, 0] * plane_z / NZ) * jnp.cos(math.pi * orders[mode, 1] * row_x / NX)
        wave = wave * jnp.cos(math.pi * orders[mode, 2] * column_y / NY)
        smooth = smooth + weights[mode] * wave
    return (sign * level + smooth + noise).astype(jnp.float32)


def with_ends(result, key, smallest, largest):
    place = [jax.random.randint(jax.random.fold_in(key, axis), (), 0, length) for axis, length in enumerate(result.shape)]
    main_axis = result.shape.index(max(result.shape))
    next_to = place[:main_axis] + [(place[main_axis] + 1) % result.shape[main_axis]] + place[main_axis + 1:]
    return result.at[tuple(place)].set(smallest).at[tuple(next_to)].set(largest)


def setup_inputs(seed: int = 0) -> dict:
    arg_keys = jax.random.split(jax.random.key(seed), 5)
    potential = draw_potential(jax.random.fold_in(arg_keys[4], 71), 0)
    tissue_mask = draw_tissue_mask(jax.random.fold_in(arg_keys[4], 71), 0)
    layer_index = with_ends(jax.random.randint(arg_keys[2], (NZ,), 0, LAYERS), jax.random.fold_in(arg_keys[2], 1), 0, LAYERS - 1).astype(jnp.int32)
    source = draw_source(jax.random.fold_in(arg_keys[4], 71), 0)
    return dict(potential=potential, tissue_mask=tissue_mask, layer_index=layer_index, source=source)


OFFSETS = [(0, 1, 0), (0, 0, 1), (1, 0, 0), (0, 1, 1), (0, 1, -1), (1, 1, 0), (-1, 1, 0), (1, 0, 1), (-1, 0, 1)]
bulk_long = 7.99
bulk_trans = 2.55
intra_long = 1.74
intra_trans = 0.19
bath_sigma = 5.0


def tensor_table(layers, longitudinal, transverse):
    depth = jnp.arange(layers, dtype=jnp.float32) / (layers - 1)
    helix = (math.pi / 3.0) * (1.0 - 2.0 * depth)
    tilted = 0.35 * jnp.cos(math.pi * depth)
    fiber_x = jnp.cos(tilted) * jnp.cos(helix)
    fiber_y = jnp.cos(tilted) * jnp.sin(helix)
    fiber_z = jnp.sin(tilted)
    spread = longitudinal - transverse
    s_xx = transverse + spread * fiber_x * fiber_x
    s_yy = transverse + spread * fiber_y * fiber_y
    s_zz = transverse + spread * fiber_z * fiber_z
    s_xy = spread * fiber_x * fiber_y
    s_xz = spread * fiber_x * fiber_z
    s_yz = spread * fiber_y * fiber_z
    columns = [s_xx - jnp.abs(s_xy) - jnp.abs(s_xz), s_yy - jnp.abs(s_xy) - jnp.abs(s_yz),
               s_zz - jnp.abs(s_xz) - jnp.abs(s_yz), jnp.maximum(s_xy, 0.0), jnp.maximum(-s_xy, 0.0),
               jnp.maximum(s_xz, 0.0), jnp.maximum(-s_xz, 0.0), jnp.maximum(s_yz, 0.0), jnp.maximum(-s_yz, 0.0)]
    return jnp.stack(columns, axis=1).astype(jnp.float32)


def window(array, offset, extent):
    return array[1 + offset[0]:1 + offset[0] + extent[0], 1 + offset[1]:1 + offset[1] + extent[1],
                 1 + offset[2]:1 + offset[2] + extent[2]]


def cell_weight(planes, column, tissue_pad, bath_pad):
    weight = tissue_pad * planes[:, column][:, None, None]
    if bath_pad is not None and column < 3:
        weight = weight + bath_sigma * bath_pad
    return weight


def edge_pair(weight, medium_pad, offset, extent):
    backward = (-offset[0], -offset[1], -offset[2])
    centre = window(medium_pad, (0, 0, 0), extent)
    own_weight = window(weight, (0, 0, 0), extent)
    forward_edge = centre * window(medium_pad, offset, extent) * (0.5 * (own_weight + window(weight, offset, extent)))
    backward_edge = centre * window(medium_pad, backward, extent) * (0.5 * (own_weight + window(weight, backward, extent)))
    return forward_edge, backward_edge


def operate(field, planes, tissue_pad, bath_pad, medium_pad):
    extent = field.shape
    field_pad = jnp.pad(field, 1)
    summed = jnp.zeros(extent, jnp.float32)
    for column, offset in enumerate(OFFSETS):
        backward = (-offset[0], -offset[1], -offset[2])
        weight = cell_weight(planes, column, tissue_pad, bath_pad)
        forward_edge, backward_edge = edge_pair(weight, medium_pad, offset, extent)
        summed = summed + forward_edge * (field - window(field_pad, offset, extent)) + backward_edge * (field - window(field_pad, backward, extent))
    return summed


def reference(potential, tissue_mask, layer_index, source):
    extent = tissue_mask.shape
    mask_pad = jnp.pad(tissue_mask, 1)
    layer_pad = jnp.pad(layer_index, 1)
    tissue_pad = (mask_pad == 2).astype(jnp.float32)
    bath_pad = (mask_pad == 1).astype(jnp.float32)
    inside_pad = (mask_pad > 0).astype(jnp.float32)
    inside = window(inside_pad, (0, 0, 0), extent)
    bulk_planes = tensor_table(LAYERS, bulk_long, bulk_trans)[layer_pad]
    intra_planes = tensor_table(LAYERS, intra_long, intra_trans)[layer_pad]
    diagonal = jnp.zeros(extent, jnp.float32)
    for column, offset in enumerate(OFFSETS):
        weight = cell_weight(bulk_planes, column, tissue_pad, bath_pad)
        forward_edge, backward_edge = edge_pair(weight, inside_pad, offset, extent)
        diagonal = diagonal + forward_edge + backward_edge
    jacobi = inside / jnp.maximum(diagonal, 1.0)
    rhs = -operate(potential, intra_planes, tissue_pad, None, tissue_pad) + inside * source
    count = jnp.sum(inside)
    residual = rhs - inside * (jnp.sum(rhs) / count)

    def precondition(current):
        scaled = jacobi * current
        return scaled - inside * (jnp.sum(scaled) / count)

    solution = jnp.zeros(extent, jnp.float32)
    precond = precondition(residual)
    direction = precond
    rz_now = jnp.sum(residual * precond)
    for step in range(ITERS):
        image = operate(direction, bulk_planes, tissue_pad, bath_pad, inside_pad)
        alpha = rz_now / jnp.sum(direction * image)
        solution = solution + alpha * direction
        residual = residual - alpha * image
        if step + 1 < ITERS:
            precond = precondition(residual)
            rz_next = jnp.sum(residual * precond)
            direction = precond + (rz_next / rz_now) * direction
            rz_now = rz_next
    return solution, residual
```

```python
import functools
import math

import jax
import jax.numpy as jnp
from jax import lax
from jax.experimental import pallas as pl
from jax.experimental.pallas import tpu as pltpu
from jax.sharding import PartitionSpec as P

ITERS = 8
DEPTH = ITERS + 1
LAYERS = 16
AXES = ("gx", "gy", "gz")

OFFSETS = [
    (0, 1, 0),
    (0, 0, 1),
    (1, 0, 0),
    (0, 1, 1),
    (0, 1, -1),
    (1, 1, 0),
    (-1, 1, 0),
    (1, 0, 1),
    (-1, 0, 1),
]
bulk_long = 7.99
bulk_trans = 2.55
intra_long = 1.74
intra_trans = 0.19
bath_sigma = 5.0


def tensor_table(layers, longitudinal, transverse):
    depth = jnp.arange(layers, dtype=jnp.float32) / (layers - 1)
    helix = math.pi / 3.0 * (1.0 - 2.0 * depth)
    tilted = 0.35 * jnp.cos(math.pi * depth)
    fiber_x = jnp.cos(tilted) * jnp.cos(helix)
    fiber_y = jnp.cos(tilted) * jnp.sin(helix)
    fiber_z = jnp.sin(tilted)
    spread = longitudinal - transverse
    s_xx = transverse + spread * fiber_x * fiber_x
    s_yy = transverse + spread * fiber_y * fiber_y
    s_zz = transverse + spread * fiber_z * fiber_z
    s_xy = spread * fiber_x * fiber_y
    s_xz = spread * fiber_x * fiber_z
    s_yz = spread * fiber_y * fiber_z
    columns = [
        s_xx - jnp.abs(s_xy) - jnp.abs(s_xz),
        s_yy - jnp.abs(s_xy) - jnp.abs(s_yz),
        s_zz - jnp.abs(s_xz) - jnp.abs(s_yz),
        jnp.maximum(s_xy, 0.0),
        jnp.maximum(-s_xy, 0.0),
        jnp.maximum(s_xz, 0.0),
        jnp.maximum(-s_xz, 0.0),
        jnp.maximum(s_yz, 0.0),
        jnp.maximum(-s_yz, 0.0),
    ]
    return jnp.stack(columns, axis=1)


def shifted(value, axis, hop):
    count = lax.axis_size(axis)
    pairs = [(i + hop, i) for i in range(count) if 0 <= i + hop < count]
    return lax.ppermute(value, axis, pairs)


def framed(value, axis, dim, multiple):
    count, length = lax.axis_size(axis), value.shape[dim]
    if count == 1:
        return value
    if count == 2 and 2 * length <= length + 2 * DEPTH and multiple == 1:
        other = lax.ppermute(value, axis, [(0, 1), (1, 0)])
        return jnp.concatenate([value, other], axis=dim)
    after, before = [], []
    left, hop = DEPTH, 1
    while left > 0:
        width = min(left, length)
        if hop < count:
            after.append(
                shifted(lax.slice_in_dim(value, 0, width, axis=dim), axis, hop)
            )
            before.insert(
                0, shifted(lax.slice_in_dim(value, length - width, length, axis=dim), axis, -hop)
            )
        else:
            shape = list(value.shape)
            shape[dim] = width
            after.append(jnp.zeros(shape, value.dtype))
            before.insert(0, jnp.zeros(shape, value.dtype))
        left, hop = left - width, hop + 1
    gap = -(length + 2 * DEPTH) % multiple
    shape = list(value.shape)
    shape[dim] = gap
    middle = [jnp.zeros(shape, value.dtype)] if gap else []
    return jnp.concatenate([value] + after + middle + before, axis=dim)


def fields_around(ref, here, above, below, rows, lanes):
    def along_x(value, step):
        return pltpu.roll(value, (-step) % rows, 0)

    def along_y(value, step):
        return pltpu.roll(value, (-step) % lanes, 1)

    for dz, plane in ((0, here), (1, above), (-1, below)):
        value = ref[plane]
        if dz:
            yield (dz, 0, 0), value
        for step in (1, -1):
            yield (dz, step, 0), along_x(value, step)
        for step in (1, -1):
            moved = along_y(value, step)
            yield (dz, 0, step), moved
            if dz == 0:
                for other in (1, -1):
                    yield (0, other, step), along_x(moved, other)


SLOT = {}
for _column, _offset in enumerate(OFFSETS):
    SLOT[_offset] = (_column, 2 * _column)
    SLOT[tuple(-o for o in _offset)] = (_column, 2 * _column + 1)


def powers_kernel(extent, table, stats, mask, potential, source, basis, scale, dots,
                  weights, spare, first, second, jac):
    planes, rows, lanes = mask.shape
    nz, nx, ny = extent
    mean_rhs = stats[0]

    def neighbours(plane):
        above = jnp.where(plane + 1 == planes, 0, plane + 1)
        below = jnp.where(plane == 0, planes - 1, plane - 1)
        return above, below

    def setup(plane, carry):
        above, below = neighbours(plane)
        labels = mask[plane]
        tissue = jnp.where(labels == 2.0, 1.0, 0.0)
        bath = jnp.where(labels == 1.0, 1.0, 0.0)
        inside = tissue + bath
        volts = potential[plane]
        total = jnp.zeros((rows, lanes), jnp.float32)
        image = jnp.zeros((rows, lanes), jnp.float32)
        pairs = zip(
            fields_around(mask, plane, above, below, rows, lanes),
            fields_around(potential, plane, above, below, rows, lanes),
        )
        for (offset, label), (_, volt) in pairs:
            column, slot = SLOT[offset]
            beyond = {0: plane, 1: above, -1: below}[offset[0]]
            link = 0.5
            if offset[0] == 1:
                link = 0.5 * table[plane, 18]
            if offset[0] == -1:
                link = 0.5 * table[below, 18]
            their_tissue = jnp.where(label == 2.0, 1.0, 0.0)
            g_here, g_there = table[plane, column] * link, table[beyond, column] * link
            weight = tissue * g_here
            if column < 3:
                their_bath = jnp.where(label == 1.0, 1.0, 0.0)
                sigma = bath_sigma * link
                weight = inside * (
                    jnp.where(label > 0.0, weight + bath * sigma, 0.0)
                    + (their_tissue * g_there + their_bath * sigma)
                )
            else:
                weight = inside * (jnp.where(label > 0.0, weight, 0.0) + their_tissue * g_there)
            weights[slot, plane] = weight
            total = total + weight
            intra = (table[plane, 9 + column] + table[beyond, 9 + column]) * link
            image = image + (tissue * their_tissue * intra) * (volts - volt)
        bounded = jnp.maximum(total, 1.0)
        jacobi = inside / bounded
        jac[plane] = jacobi + jacobi
        spare[plane] = inside * (1.0 - jacobi * total)
        first[plane] = jacobi * (inside * source[plane] - image - inside * mean_rhs)

        @pl.when(plane < nz)
        def _():
            scale[plane] = (inside * bounded)[:nx, :ny]

        return carry

    lax.fori_loop(0, planes, setup, 0)

    def record(step, now, before):
        rowsum = jnp.zeros((1, ny), jnp.float32)
        square, cross, plain = rowsum, rowsum, rowsum
        for plane in range(nz):
            value = now[plane, 0:nx, 0:ny]
            basis[step, plane] = value
            weighted = value * scale[plane]
            square = square + jnp.sum(weighted * value, axis=0, keepdims=True)
            if step:
                past = basis[step - 1, plane]
                cross = cross + jnp.sum(weighted * past, axis=0, keepdims=True)
            plain = plain + jnp.sum(value, axis=0, keepdims=True)
        if step < ITERS:
            dots[pl.ds(2 * step, 1)] = square
            dots[pl.ds(2 * ITERS + step, 1)] = plain
        if step:
            dots[pl.ds(2 * step - 1, 1)] = cross

    record(0, first, None)

    def apply(now, old, start):
        def one(plane, carry):
            above, below = neighbours(plane)
            total = jnp.zeros((rows, lanes), jnp.float32)
            for offset, value in fields_around(now, plane, above, below, rows, lanes):
                total = total + weights[SLOT[offset][1], plane] * value
            if start:
                old[plane] = 0.5 * jac[plane] * total + spare[plane] * now[plane]
            else:
                old[plane] = (
                    jac[plane] * total + 2.0 * spare[plane] * now[plane] - old[plane]
                )
            return carry

        lax.fori_loop(0, planes, one, 0)

    now, old = first, second
    for step in range(1, ITERS + 1):
        apply(now, old, step == 1)
        now, old = old, now
        record(step, now, old)


def combine_kernel(raw, count, basis, scale, phi, residual):
    nz = scale.shape[0]
    lane = lax.broadcasted_iota(jnp.int32, (1, 128), 1)
    sums = raw[...]

    def pick(vector, index):
        return jnp.sum(jnp.where(lane == index, vector, 0.0), axis=1, keepdims=True)

    def left(vector):
        return pltpu.roll(vector, 127, 1)

    def right(vector):
        return pltpu.roll(vector, 1, 1)

    mu0, mu1 = pick(sums, 0), pick(sums, 1)
    mu = jnp.where(lane < 2, sums, 2.0 * sums - jnp.where(lane % 2 == 0, mu0, mu1))
    mu = jnp.where(lane < 2 * ITERS, mu, 0.0)
    ones = pltpu.roll(sums, 128 - 2 * ITERS, 1)
    y = jnp.where(lane == 0, 1.0, 0.0)
    p = y
    m_y, m_p = mu, mu
    x = jnp.zeros((1, 128), jnp.float32)
    rz = mu0
    for step in range(ITERS):
        h_p = p - 0.5 * (left(p) + jnp.where(lane == 1, 2.0, 1.0) * right(p))
        h_p = jnp.where(lane <= ITERS, h_p, 0.0)
        before = jnp.where(lane == 0, left(m_p), right(m_p))
        m_h = m_p - 0.5 * (left(m_p) + before)
        alpha = rz / jnp.sum(jnp.where(lane < ITERS, p * m_h, 0.0), axis=1, keepdims=True)
        x = x + alpha * p
        y = y - alpha * h_p
        m_y = m_y - alpha * m_h
        if step + 1 < ITERS:
            rz_next = jnp.sum(jnp.where(lane < ITERS, y * m_y, 0.0), axis=1, keepdims=True)
            beta = rz_next / rz
            p = y + beta * p
            m_p = m_y + beta * m_p
            rz = rz_next
    mean = jnp.sum(jnp.where(lane < ITERS, x * ones, 0.0), axis=1, keepdims=True) / count[0]
    xs = [pick(x, j) for j in range(ITERS)]
    ys = [pick(y, j) for j in range(ITERS + 1)]

    def one(plane, carry):
        weight = scale[plane]
        total = jnp.where(weight > 0.0, -mean, 0.0)
        rest = ys[ITERS] * basis[ITERS, plane]
        for j in range(ITERS):
            value = basis[j, plane]
            total = total + xs[j] * value
            rest = rest + ys[j] * value
        phi[plane] = total
        residual[plane] = weight * rest
        return carry

    lax.fori_loop(0, nz, one, 0)


def body(potential, tissue_mask, layer_index, source):
    extent = tissue_mask.shape
    nz = extent[0]
    labels = tissue_mask.astype(jnp.float32)
    own_inside = (labels > 0.0).astype(jnp.float32)
    count, rhs_total = lax.psum(
        (jnp.sum(own_inside), jnp.sum(own_inside * source)), AXES
    )
    packed = jnp.stack([labels, potential, source], axis=1)
    packed = framed(packed, "gz", 0, 1)
    packed = framed(packed, "gx", 2, 8)
    packed = framed(packed, "gy", 3, 128)
    layers = framed(layer_index, "gz", 0, 1)
    planes = layers.shape[0]
    selector = (layers[:, None] == jnp.arange(LAYERS, dtype=jnp.int32)[None, :]).astype(
        jnp.float32
    )
    tables = jnp.concatenate(
        [
            tensor_table(LAYERS, bulk_long, bulk_trans),
            tensor_table(LAYERS, intra_long, intra_trans),
        ],
        axis=1,
    )
    table = jnp.dot(selector, tables, precision=lax.Precision.HIGHEST)
    size = lax.axis_size("gz")
    link = jnp.ones((planes, 1), jnp.float32)
    if planes == size * nz:
        place = (lax.axis_index("gz") * nz + jnp.arange(planes)) % planes
        link = (place + 1 < planes).astype(jnp.float32)[:, None]
    table = jnp.concatenate([table, link], axis=1)
    frame = (planes,) + packed.shape[2:]
    smem = pl.BlockSpec(memory_space=pltpu.SMEM)
    vmem = pl.BlockSpec(memory_space=pltpu.VMEM)
    basis, scale, dots = pl.pallas_call(
        functools.partial(powers_kernel, extent),
        out_shape=(
            jax.ShapeDtypeStruct((ITERS + 1,) + extent, jnp.float32),
            jax.ShapeDtypeStruct(extent, jnp.float32),
            jax.ShapeDtypeStruct((3 * ITERS, extent[2]), jnp.float32),
        ),
        in_specs=[smem, smem, vmem, vmem, vmem],
        out_specs=(vmem, vmem, vmem),
        scratch_shapes=[pltpu.VMEM((18,) + frame, jnp.float32)]
        + [pltpu.VMEM(frame, jnp.float32)] * 4,
        compiler_params=pltpu.CompilerParams(vmem_limit_bytes=60 * 1024 * 1024),
    )(table, (rhs_total / count)[None], packed[:, 0], packed[:, 1], packed[:, 2])
    sums = lax.psum(jnp.sum(dots, axis=1), AXES)
    raw = jnp.zeros((1, 128), jnp.float32).at[0, : 3 * ITERS].set(sums)
    return tuple(
        pl.pallas_call(
            combine_kernel,
            out_shape=(jax.ShapeDtypeStruct(extent, jnp.float32),) * 2,
            in_specs=[vmem, smem, vmem, vmem],
            out_specs=(vmem, vmem),
        )(raw, count[None], basis, scale)
    )


def solution(mesh):
    placed = (P("gz", "gx", "gy"), P("gz", "gx", "gy"), P("gz"), P("gz", "gx", "gy"))
    return jax.shard_map(
        body,
        mesh=mesh,
        in_specs=placed,
        out_specs=(P("gz", "gx", "gy"), P("gz", "gx", "gy")),
        check_vma=False,
    )
```

```python
import functools
import math

import jax
import jax.numpy as jnp
from jax import lax
from jax.experimental import pallas as pl
from jax.experimental.pallas import tpu as pltpu
from jax.sharding import PartitionSpec as P

ITERS = 8
DEPTH = ITERS + 1
LAYERS = 16
AXES = ("gx", "gy", "gz")

OFFSETS = [
    (0, 1, 0),
    (0, 0, 1),
    (1, 0, 0),
    (0, 1, 1),
    (0, 1, -1),
    (1, 1, 0),
    (-1, 1, 0),
    (1, 0, 1),
    (-1, 0, 1),
]
bulk_long = 7.99
bulk_trans = 2.55
intra_long = 1.74
intra_trans = 0.19
bath_sigma = 5.0


def tensor_table(layers, longitudinal, transverse):
    depth = jnp.arange(layers, dtype=jnp.float32) / (layers - 1)
    helix = math.pi / 3.0 * (1.0 - 2.0 * depth)
    tilted = 0.35 * jnp.cos(math.pi * depth)
    fiber_x = jnp.cos(tilted) * jnp.cos(helix)
    fiber_y = jnp.cos(tilted) * jnp.sin(helix)
    fiber_z = jnp.sin(tilted)
    spread = longitudinal - transverse
    s_xx = transverse + spread * fiber_x * fiber_x
    s_yy = transverse + spread * fiber_y * fiber_y
    s_zz = transverse + spread * fiber_z * fiber_z
    s_xy = spread * fiber_x * fiber_y
    s_xz = spread * fiber_x * fiber_z
    s_yz = spread * fiber_y * fiber_z
    columns = [
        s_xx - jnp.abs(s_xy) - jnp.abs(s_xz),
        s_yy - jnp.abs(s_xy) - jnp.abs(s_yz),
        s_zz - jnp.abs(s_xz) - jnp.abs(s_yz),
        jnp.maximum(s_xy, 0.0),
        jnp.maximum(-s_xy, 0.0),
        jnp.maximum(s_xz, 0.0),
        jnp.maximum(-s_xz, 0.0),
        jnp.maximum(s_yz, 0.0),
        jnp.maximum(-s_yz, 0.0),
    ]
    return jnp.stack(columns, axis=1)


def shifted(value, axis, hop):
    count = lax.axis_size(axis)
    pairs = [(i + hop, i) for i in range(count) if 0 <= i + hop < count]
    return lax.ppermute(value, axis, pairs)


def framed(value, axis, dim, multiple):
    count, length = lax.axis_size(axis), value.shape[dim]
    if count == 1:
        return value
    if count == 2 and 2 * length <= length + 2 * DEPTH and multiple == 1:
        other = lax.ppermute(value, axis, [(0, 1), (1, 0)])
        return jnp.concatenate([value, other], axis=dim)
    after, before = [], []
    left, hop = DEPTH, 1
    while left > 0:
        width = min(left, length)
        if hop < count:
            after.append(
                shifted(lax.slice_in_dim(value, 0, width, axis=dim), axis, hop)
            )
            before.insert(
                0, shifted(lax.slice_in_dim(value, length - width, length, axis=dim), axis, -hop)
            )
        else:
            shape = list(value.shape)
            shape[dim] = width
            after.append(jnp.zeros(shape, value.dtype))
            before.insert(0, jnp.zeros(shape, value.dtype))
        left, hop = left - width, hop + 1
    gap = -(length + 2 * DEPTH) % multiple
    shape = list(value.shape)
    shape[dim] = gap
    middle = [jnp.zeros(shape, value.dtype)] if gap else []
    return jnp.concatenate([value] + after + middle + before, axis=dim)


def fields_around(ref, here, above, below, rows, lanes):
    def along_x(value, step):
        return pltpu.roll(value, (-step) % rows, 0)

    def along_y(value, step):
        return pltpu.roll(value, (-step) % lanes, 1)

    for dz, plane in ((0, here), (1, above), (-1, below)):
        value = ref[plane]
        if dz:
            yield (dz, 0, 0), value
        for step in (1, -1):
            yield (dz, step, 0), along_x(value, step)
        for step in (1, -1):
            moved = along_y(value, step)
            yield (dz, 0, step), moved
            if dz == 0:
                for other in (1, -1):
                    yield (0, other, step), along_x(moved, other)


SLOT = {}
for _column, _offset in enumerate(OFFSETS):
    SLOT[_offset] = (_column, 2 * _column)
    SLOT[tuple(-o for o in _offset)] = (_column, 2 * _column + 1)


def grid_kernel(extent, sizes, table, mask, potential, source, phi, residual,
                basis, scale, dots, weights, spare, first, second, jac,
                own_row, early, final_row, late, sends, early_recv, late_recv):
    planes, rows, lanes = mask.shape
    nz, nx, ny = extent
    peers = math.prod(sizes)
    me = 0
    for axis, size in zip(AXES, sizes):
        me = me * size + lax.axis_index(axis)

    def device(index):
        return (index // (sizes[1] * sizes[2]), index // sizes[2] % sizes[1], index % sizes[2])

    def peer(k):
        return lax.rem(me + k, peers)

    barrier = pltpu.get_barrier_semaphore()

    def greet(k, carry):
        pl.semaphore_signal(
            barrier, inc=1, device_id=device(peer(k)), device_id_type=pl.DeviceIdType.MESH
        )
        return carry

    lax.fori_loop(1, peers, greet, 0)

    def spread(row, gathered, recv):
        def one(k, carry):
            pltpu.make_async_remote_copy(
                src_ref=row, dst_ref=gathered.at[me], send_sem=sends.at[k],
                recv_sem=recv.at[me], device_id=device(peer(k)),
                device_id_type=pl.DeviceIdType.MESH,
            ).start()
            return carry

        lax.fori_loop(1, peers, one, 0)

    def collect(row, gathered, recv):
        def one(k, carry):
            other = peer(k)
            copy = pltpu.make_async_remote_copy(
                src_ref=row, dst_ref=gathered.at[other], send_sem=sends.at[k],
                recv_sem=recv.at[other], device_id=device(other),
                device_id_type=pl.DeviceIdType.MESH,
            )
            copy.wait_recv()
            copy.wait_send()
            return carry

        lax.fori_loop(1, peers, one, 0)
        gathered[me] = row[...]
        return jnp.sum(gathered[...], axis=0)

    lane = lax.broadcasted_iota(jnp.int32, (1, 128), 1)

    def pick(vector, index):
        return jnp.sum(jnp.where(lane == index, vector, 0.0), axis=1, keepdims=True)

    cells = jnp.zeros((1, ny), jnp.float32)
    injected = jnp.zeros((1, ny), jnp.float32)
    for plane in range(nz):
        own_inside = jnp.where(mask[plane, 0:nx, 0:ny] > 0.0, 1.0, 0.0)
        cells = cells + jnp.sum(own_inside, axis=0, keepdims=True)
        injected = injected + jnp.sum(
            own_inside * source[plane, 0:nx, 0:ny], axis=0, keepdims=True
        )
    cells = jnp.sum(cells, axis=1, keepdims=True)
    injected = jnp.sum(injected, axis=1, keepdims=True)
    own_row[...] = jnp.where(lane == 0, cells, jnp.where(lane == 1, injected, 0.0))

    def neighbours(plane):
        above = jnp.where(plane + 1 == planes, 0, plane + 1)
        below = jnp.where(plane == 0, planes - 1, plane - 1)
        return above, below

    def setup(plane, carry):
        above, below = neighbours(plane)
        labels = mask[plane]
        tissue = jnp.where(labels == 2.0, 1.0, 0.0)
        bath = jnp.where(labels == 1.0, 1.0, 0.0)
        inside = tissue + bath
        volts = potential[plane]
        total = jnp.zeros((rows, lanes), jnp.float32)
        image = jnp.zeros((rows, lanes), jnp.float32)
        pairs = zip(
            fields_around(mask, plane, above, below, rows, lanes),
            fields_around(potential, plane, above, below, rows, lanes),
        )
        for (offset, label), (_, volt) in pairs:
            column, slot = SLOT[offset]
            beyond = {0: plane, 1: above, -1: below}[offset[0]]
            link = 0.5
            if offset[0] == 1:
                link = 0.5 * table[plane, 18]
            if offset[0] == -1:
                link = 0.5 * table[below, 18]
            their_tissue = jnp.where(label == 2.0, 1.0, 0.0)
            g_here, g_there = table[plane, column] * link, table[beyond, column] * link
            weight = tissue * g_here
            if column < 3:
                their_bath = jnp.where(label == 1.0, 1.0, 0.0)
                sigma = bath_sigma * link
                weight = inside * (
                    jnp.where(label > 0.0, weight + bath * sigma, 0.0)
                    + (their_tissue * g_there + their_bath * sigma)
                )
            else:
                weight = inside * (jnp.where(label > 0.0, weight, 0.0) + their_tissue * g_there)
            weights[slot, plane] = weight
            total = total + weight
            intra = (table[plane, 9 + column] + table[beyond, 9 + column]) * link
            image = image + (tissue * their_tissue * intra) * (volts - volt)
        bounded = jnp.maximum(total, 1.0)
        jacobi = inside / bounded
        jac[plane] = jacobi + jacobi
        spare[plane] = inside * (1.0 - jacobi * total)
        first[plane] = jacobi * (inside * source[plane] - image)

        @pl.when(plane < nz)
        def _():
            scale[plane] = (inside * bounded)[:nx, :ny]

        return carry

    lax.fori_loop(0, planes // 2, setup, 0)
    pl.semaphore_wait(barrier, peers - 1)
    spread(own_row, early, early_recv)
    lax.fori_loop(planes // 2, planes, setup, 0)
    totals = collect(own_row, early, early_recv)
    count = pick(totals, 0)
    mean_rhs = pick(totals, 1) / count

    def centre(plane, carry):
        first[plane] = first[plane] - 0.5 * jac[plane] * mean_rhs
        return carry

    lax.fori_loop(0, planes, centre, 0)

    def record(step, now, before):
        rowsum = jnp.zeros((1, ny), jnp.float32)
        square, cross, plain = rowsum, rowsum, rowsum
        for plane in range(nz):
            value = now[plane, 0:nx, 0:ny]
            basis[step, plane] = value
            weighted = value * scale[plane]
            square = square + jnp.sum(weighted * value, axis=0, keepdims=True)
            if step:
                past = basis[step - 1, plane]
                cross = cross + jnp.sum(weighted * past, axis=0, keepdims=True)
            plain = plain + jnp.sum(value, axis=0, keepdims=True)
        if step < ITERS:
            dots[pl.ds(2 * step, 1)] = square
            dots[pl.ds(2 * ITERS + step, 1)] = plain
        if step:
            dots[pl.ds(2 * step - 1, 1)] = cross

    record(0, first, None)

    def apply(now, old, start):
        def one(plane, carry):
            above, below = neighbours(plane)
            total = jnp.zeros((rows, lanes), jnp.float32)
            for offset, value in fields_around(now, plane, above, below, rows, lanes):
                total = total + weights[SLOT[offset][1], plane] * value
            if start:
                old[plane] = 0.5 * jac[plane] * total + spare[plane] * now[plane]
            else:
                old[plane] = (
                    jac[plane] * total + 2.0 * spare[plane] * now[plane] - old[plane]
                )
            return carry

        lax.fori_loop(0, planes, one, 0)

    now, old = first, second
    for step in range(1, ITERS + 1):
        apply(now, old, step == 1)
        now, old = old, now
        record(step, now, old)

    partial = jnp.sum(dots[...], axis=1, keepdims=True)
    diagonal = lax.broadcasted_iota(jnp.int32, (3 * ITERS, 128), 0) == lax.broadcasted_iota(
        jnp.int32, (3 * ITERS, 128), 1
    )
    final_row[...] = jnp.sum(jnp.where(diagonal, partial, 0.0), axis=0, keepdims=True)
    spread(final_row, late, late_recv)
    sums = collect(final_row, late, late_recv)

    def left(vector):
        return pltpu.roll(vector, 127, 1)

    def right(vector):
        return pltpu.roll(vector, 1, 1)

    mu0, mu1 = pick(sums, 0), pick(sums, 1)
    mu = jnp.where(lane < 2, sums, 2.0 * sums - jnp.where(lane % 2 == 0, mu0, mu1))
    mu = jnp.where(lane < 2 * ITERS, mu, 0.0)
    ones = pltpu.roll(sums, 128 - 2 * ITERS, 1)
    y = jnp.where(lane == 0, 1.0, 0.0)
    p = y
    m_y, m_p = mu, mu
    x = jnp.zeros((1, 128), jnp.float32)
    rz = mu0
    for step in range(ITERS):
        h_p = p - 0.5 * (left(p) + jnp.where(lane == 1, 2.0, 1.0) * right(p))
        h_p = jnp.where(lane <= ITERS, h_p, 0.0)
        before = jnp.where(lane == 0, left(m_p), right(m_p))
        m_h = m_p - 0.5 * (left(m_p) + before)
        alpha = rz / jnp.sum(jnp.where(lane < ITERS, p * m_h, 0.0), axis=1, keepdims=True)
        x = x + alpha * p
        y = y - alpha * h_p
        m_y = m_y - alpha * m_h
        if step + 1 < ITERS:
            rz_next = jnp.sum(jnp.where(lane < ITERS, y * m_y, 0.0), axis=1, keepdims=True)
            beta = rz_next / rz
            p = y + beta * p
            m_p = m_y + beta * m_p
            rz = rz_next
    mean = jnp.sum(jnp.where(lane < ITERS, x * ones, 0.0), axis=1, keepdims=True) / count
    xs = [pick(x, j) for j in range(ITERS)]
    ys = [pick(y, j) for j in range(ITERS + 1)]

    def one(plane, carry):
        weight = scale[plane]
        total = jnp.where(weight > 0.0, -mean, 0.0)
        rest = ys[ITERS] * basis[ITERS, plane]
        for j in range(ITERS):
            value = basis[j, plane]
            total = total + xs[j] * value
            rest = rest + ys[j] * value
        phi[plane] = total
        residual[plane] = weight * rest
        return carry

    lax.fori_loop(0, nz, one, 0)


def body(potential, tissue_mask, layer_index, source):
    extent = tissue_mask.shape
    nz = extent[0]
    labels = tissue_mask.astype(jnp.float32)
    packed = jnp.stack([labels, potential, source], axis=1)
    packed = framed(packed, "gz", 0, 1)
    packed = framed(packed, "gx", 2, 8)
    packed = framed(packed, "gy", 3, 128)
    layers = framed(layer_index, "gz", 0, 1)
    planes = layers.shape[0]
    selector = (layers[:, None] == jnp.arange(LAYERS, dtype=jnp.int32)[None, :]).astype(
        jnp.float32
    )
    tables = jnp.concatenate(
        [
            tensor_table(LAYERS, bulk_long, bulk_trans),
            tensor_table(LAYERS, intra_long, intra_trans),
        ],
        axis=1,
    )
    table = jnp.dot(selector, tables, precision=lax.Precision.HIGHEST)
    size = lax.axis_size("gz")
    link = jnp.ones((planes, 1), jnp.float32)
    if planes == size * nz:
        place = (lax.axis_index("gz") * nz + jnp.arange(planes)) % planes
        link = (place + 1 < planes).astype(jnp.float32)[:, None]
    table = jnp.concatenate([table, link], axis=1)
    frame = (planes,) + packed.shape[2:]
    smem = pl.BlockSpec(memory_space=pltpu.SMEM)
    vmem = pl.BlockSpec(memory_space=pltpu.VMEM)
    sizes = tuple(lax.axis_size(axis) for axis in AXES)
    peers = math.prod(sizes)
    row = pltpu.VMEM((1, 128), jnp.float32)
    gathered = pltpu.VMEM((peers, 1, 128), jnp.float32)
    return tuple(
        pl.pallas_call(
            functools.partial(grid_kernel, extent, sizes),
            out_shape=(jax.ShapeDtypeStruct(extent, jnp.float32),) * 2,
            in_specs=[smem, vmem, vmem, vmem],
            out_specs=(vmem, vmem),
            scratch_shapes=[
                pltpu.VMEM((ITERS + 1,) + extent, jnp.float32),
                pltpu.VMEM(extent, jnp.float32),
                pltpu.VMEM((3 * ITERS, extent[2]), jnp.float32),
                pltpu.VMEM((18,) + frame, jnp.float32),
            ]
            + [pltpu.VMEM(frame, jnp.float32)] * 4
            + [row, gathered, row, gathered]
            + [pltpu.SemaphoreType.DMA((peers,))] * 3,
            compiler_params=pltpu.CompilerParams(
                vmem_limit_bytes=60 * 1024 * 1024, collective_id=0, has_side_effects=True
            ),
        )(table, packed[:, 0], packed[:, 1], packed[:, 2])
    )


def solution(mesh):
    placed = (P("gz", "gx", "gy"), P("gz", "gx", "gy"), P("gz"), P("gz", "gx", "gy"))
    return jax.shard_map(
        body,
        mesh=mesh,
        in_specs=placed,
        out_specs=(P("gz", "gx", "gy"), P("gz", "gx", "gy")),
        check_vma=False,
    )
```

```python
import functools
import math

import jax
import jax.numpy as jnp
from jax import lax
from jax.experimental import pallas as pl
from jax.experimental.pallas import tpu as pltpu
from jax.sharding import PartitionSpec as P

ITERS = 8
DEPTH = ITERS + 1
LAYERS = 16
AXES = ("gx", "gy", "gz")

OFFSETS = [
    (0, 1, 0),
    (0, 0, 1),
    (1, 0, 0),
    (0, 1, 1),
    (0, 1, -1),
    (1, 1, 0),
    (-1, 1, 0),
    (1, 0, 1),
    (-1, 0, 1),
]
bulk_long = 7.99
bulk_trans = 2.55
intra_long = 1.74
intra_trans = 0.19
bath_sigma = 5.0


def tensor_table(layers, longitudinal, transverse):
    depth = jnp.arange(layers, dtype=jnp.float32) / (layers - 1)
    helix = math.pi / 3.0 * (1.0 - 2.0 * depth)
    tilted = 0.35 * jnp.cos(math.pi * depth)
    fiber_x = jnp.cos(tilted) * jnp.cos(helix)
    fiber_y = jnp.cos(tilted) * jnp.sin(helix)
    fiber_z = jnp.sin(tilted)
    spread = longitudinal - transverse
    s_xx = transverse + spread * fiber_x * fiber_x
    s_yy = transverse + spread * fiber_y * fiber_y
    s_zz = transverse + spread * fiber_z * fiber_z
    s_xy = spread * fiber_x * fiber_y
    s_xz = spread * fiber_x * fiber_z
    s_yz = spread * fiber_y * fiber_z
    columns = [
        s_xx - jnp.abs(s_xy) - jnp.abs(s_xz),
        s_yy - jnp.abs(s_xy) - jnp.abs(s_yz),
        s_zz - jnp.abs(s_xz) - jnp.abs(s_yz),
        jnp.maximum(s_xy, 0.0),
        jnp.maximum(-s_xy, 0.0),
        jnp.maximum(s_xz, 0.0),
        jnp.maximum(-s_xz, 0.0),
        jnp.maximum(s_yz, 0.0),
        jnp.maximum(-s_yz, 0.0),
    ]
    return jnp.stack(columns, axis=1)


def shifted(value, axis, hop):
    count = lax.axis_size(axis)
    pairs = [(i + hop, i) for i in range(count) if 0 <= i + hop < count]
    return lax.ppermute(value, axis, pairs)


def framed(value, axis, dim, multiple):
    count, length = lax.axis_size(axis), value.shape[dim]
    if count == 1:
        return value
    if count == 2 and 2 * length <= length + 2 * DEPTH and multiple == 1:
        other = lax.ppermute(value, axis, [(0, 1), (1, 0)])
        return jnp.concatenate([value, other], axis=dim)
    after, before = [], []
    left, hop = DEPTH, 1
    while left > 0:
        width = min(left, length)
        if hop < count:
            after.append(
                shifted(lax.slice_in_dim(value, 0, width, axis=dim), axis, hop)
            )
            before.insert(
                0, shifted(lax.slice_in_dim(value, length - width, length, axis=dim), axis, -hop)
            )
        else:
            shape = list(value.shape)
            shape[dim] = width
            after.append(jnp.zeros(shape, value.dtype))
            before.insert(0, jnp.zeros(shape, value.dtype))
        left, hop = left - width, hop + 1
    gap = -(length + 2 * DEPTH) % multiple
    shape = list(value.shape)
    shape[dim] = gap
    middle = [jnp.zeros(shape, value.dtype)] if gap else []
    return jnp.concatenate([value] + after + middle + before, axis=dim)


def fields_around(ref, here, above, below, rows, lanes):
    def along_x(value, step):
        return pltpu.roll(value, (-step) % rows, 0)

    def along_y(value, step):
        return pltpu.roll(value, (-step) % lanes, 1)

    for dz, plane in ((0, here), (1, above), (-1, below)):
        value = ref[plane]
        if dz:
            yield (dz, 0, 0), value
        for step in (1, -1):
            yield (dz, step, 0), along_x(value, step)
        for step in (1, -1):
            moved = along_y(value, step)
            yield (dz, 0, step), moved
            if dz == 0:
                for other in (1, -1):
                    yield (0, other, step), along_x(moved, other)


SLOT = {}
for _column, _offset in enumerate(OFFSETS):
    SLOT[_offset] = (_column, 2 * _column)
    SLOT[tuple(-o for o in _offset)] = (_column, 2 * _column + 1)


def grid_kernel(extent, sizes, table, mask, potential, source, phi, residual,
                basis, scale, dots, weights, spare, first, second, jac,
                own_row, early, final_row, late, sends, early_recv, late_recv):
    planes, rows, lanes = mask.shape
    nz, nx, ny = extent
    held = jac.shape[1]
    keep = nx + ITERS
    peers = math.prod(sizes)
    me = 0
    for axis, size in zip(AXES, sizes):
        me = me * size + lax.axis_index(axis)

    def device(index):
        return (index // (sizes[1] * sizes[2]), index // sizes[2] % sizes[1], index % sizes[2])

    def peer(k):
        return lax.rem(me + k, peers)

    barrier = pltpu.get_barrier_semaphore()

    def greet(k, carry):
        pl.semaphore_signal(
            barrier, inc=1, device_id=device(peer(k)), device_id_type=pl.DeviceIdType.MESH
        )
        return carry

    lax.fori_loop(1, peers, greet, 0)

    def spread(row, gathered, recv):
        def one(k, carry):
            pltpu.make_async_remote_copy(
                src_ref=row, dst_ref=gathered.at[me], send_sem=sends.at[k],
                recv_sem=recv.at[me], device_id=device(peer(k)),
                device_id_type=pl.DeviceIdType.MESH,
            ).start()
            return carry

        lax.fori_loop(1, peers, one, 0)

    def collect(row, gathered, recv):
        def one(k, carry):
            other = peer(k)
            copy = pltpu.make_async_remote_copy(
                src_ref=row, dst_ref=gathered.at[other], send_sem=sends.at[k],
                recv_sem=recv.at[other], device_id=device(other),
                device_id_type=pl.DeviceIdType.MESH,
            )
            copy.wait_recv()
            copy.wait_send()
            return carry

        lax.fori_loop(1, peers, one, 0)
        gathered[me] = row[...]
        return jnp.sum(gathered[...], axis=0)

    lane = lax.broadcasted_iota(jnp.int32, (1, 128), 1)

    def pick(vector, index):
        return jnp.sum(jnp.where(lane == index, vector, 0.0), axis=1, keepdims=True)

    cells = jnp.zeros((1, ny), jnp.float32)
    injected = jnp.zeros((1, ny), jnp.float32)
    for plane in range(nz):
        own_inside = jnp.where(mask[plane, 0:nx, 0:ny] > 0.0, 1.0, 0.0)
        cells = cells + jnp.sum(own_inside, axis=0, keepdims=True)
        injected = injected + jnp.sum(
            own_inside * source[plane, 0:nx, 0:ny], axis=0, keepdims=True
        )
    cells = jnp.sum(cells, axis=1, keepdims=True)
    injected = jnp.sum(injected, axis=1, keepdims=True)
    own_row[...] = jnp.where(lane == 0, cells, jnp.where(lane == 1, injected, 0.0))

    def neighbours(plane):
        above = jnp.where(plane + 1 == planes, 0, plane + 1)
        below = jnp.where(plane == 0, planes - 1, plane - 1)
        return above, below

    def store(ref, index, value):
        if held == rows:
            ref[index] = value
        else:
            ref[(*index, slice(0, keep))] = value[:keep]
            ref[(*index, slice(keep, held))] = value[rows - held + keep :]

    def setup(plane, carry):
        above, below = neighbours(plane)
        labels = mask[plane]
        tissue = jnp.where(labels == 2.0, 1.0, 0.0)
        bath = jnp.where(labels == 1.0, 1.0, 0.0)
        inside = tissue + bath
        volts = potential[plane]
        total = jnp.zeros((rows, lanes), jnp.float32)
        image = jnp.zeros((rows, lanes), jnp.float32)
        pairs = zip(
            fields_around(mask, plane, above, below, rows, lanes),
            fields_around(potential, plane, above, below, rows, lanes),
        )
        for (offset, label), (_, volt) in pairs:
            column, slot = SLOT[offset]
            beyond = {0: plane, 1: above, -1: below}[offset[0]]
            link = 0.5
            if offset[0] == 1:
                link = 0.5 * table[plane, 18]
            if offset[0] == -1:
                link = 0.5 * table[below, 18]
            their_tissue = jnp.where(label == 2.0, 1.0, 0.0)
            g_here, g_there = table[plane, column] * link, table[beyond, column] * link
            weight = tissue * g_here
            if column < 3:
                their_bath = jnp.where(label == 1.0, 1.0, 0.0)
                sigma = bath_sigma * link
                weight = inside * (
                    jnp.where(label > 0.0, weight + bath * sigma, 0.0)
                    + (their_tissue * g_there + their_bath * sigma)
                )
            else:
                weight = inside * (jnp.where(label > 0.0, weight, 0.0) + their_tissue * g_there)
            store(weights, (slot, plane), weight)
            total = total + weight
            intra = (table[plane, 9 + column] + table[beyond, 9 + column]) * link
            image = image + (tissue * their_tissue * intra) * (volts - volt)
        bounded = jnp.maximum(total, 1.0)
        jacobi = inside / bounded
        store(jac, (plane,), jacobi + jacobi)
        store(spare, (plane,), inside * (1.0 - jacobi * total))
        store(first, (plane,), jacobi * (inside * source[plane] - image))

        @pl.when(plane < nz)
        def _():
            scale[plane] = (inside * bounded)[:nx, :ny]

        return carry

    lax.fori_loop(0, planes // 2, setup, 0)
    pl.semaphore_wait(barrier, peers - 1)
    spread(own_row, early, early_recv)
    lax.fori_loop(planes // 2, planes, setup, 0)
    totals = collect(own_row, early, early_recv)
    count = pick(totals, 0)
    mean_rhs = pick(totals, 1) / count

    def centre(plane, carry):
        first[plane] = first[plane] - 0.5 * jac[plane] * mean_rhs
        return carry

    lax.fori_loop(0, planes, centre, 0)

    def record(step, now, before):
        rowsum = jnp.zeros((1, ny), jnp.float32)
        square, cross, plain = rowsum, rowsum, rowsum
        for plane in range(nz):
            value = now[plane, 0:nx, 0:ny]
            basis[step, plane] = value
            weighted = value * scale[plane]
            square = square + jnp.sum(weighted * value, axis=0, keepdims=True)
            if step:
                past = basis[step - 1, plane]
                cross = cross + jnp.sum(weighted * past, axis=0, keepdims=True)
            plain = plain + jnp.sum(value, axis=0, keepdims=True)
        if step < ITERS:
            dots[pl.ds(2 * step, 1)] = square
            dots[pl.ds(2 * ITERS + step, 1)] = plain
        if step:
            dots[pl.ds(2 * step - 1, 1)] = cross

    record(0, first, None)

    def apply(now, old, step):
        reach = ITERS - step
        if planes == nz:
            begin, span = 0, nz
        elif planes == sizes[2] * nz:
            begin = planes - lax.axis_index("gz") * reach
            span = min(planes, nz + reach)
        else:
            begin, span = planes - reach, nz + 2 * reach

        def one(index, carry):
            plane = lax.rem(begin + index, planes)
            above, below = neighbours(plane)
            total = jnp.zeros((held, lanes), jnp.float32)
            for offset, value in fields_around(now, plane, above, below, held, lanes):
                total = total + weights[SLOT[offset][1], plane] * value
            if step == 1:
                old[plane] = 0.5 * jac[plane] * total + spare[plane] * now[plane]
            else:
                old[plane] = (
                    jac[plane] * total + 2.0 * spare[plane] * now[plane] - old[plane]
                )
            return carry

        lax.fori_loop(0, span, one, 0)

    now, old = first, second
    for step in range(1, ITERS + 1):
        apply(now, old, step)
        now, old = old, now
        record(step, now, old)

    partial = jnp.sum(dots[...], axis=1, keepdims=True)
    diagonal = lax.broadcasted_iota(jnp.int32, (3 * ITERS, 128), 0) == lax.broadcasted_iota(
        jnp.int32, (3 * ITERS, 128), 1
    )
    final_row[...] = jnp.sum(jnp.where(diagonal, partial, 0.0), axis=0, keepdims=True)
    spread(final_row, late, late_recv)
    sums = collect(final_row, late, late_recv)

    def left(vector):
        return pltpu.roll(vector, 127, 1)

    def right(vector):
        return pltpu.roll(vector, 1, 1)

    mu0, mu1 = pick(sums, 0), pick(sums, 1)
    mu = jnp.where(lane < 2, sums, 2.0 * sums - jnp.where(lane % 2 == 0, mu0, mu1))
    mu = jnp.where(lane < 2 * ITERS, mu, 0.0)
    ones = pltpu.roll(sums, 128 - 2 * ITERS, 1)
    y = jnp.where(lane == 0, 1.0, 0.0)
    p = y
    m_y, m_p = mu, mu
    x = jnp.zeros((1, 128), jnp.float32)
    rz = mu0
    for step in range(ITERS):
        h_p = p - 0.5 * (left(p) + jnp.where(lane == 1, 2.0, 1.0) * right(p))
        h_p = jnp.where(lane <= ITERS, h_p, 0.0)
        before = jnp.where(lane == 0, left(m_p), right(m_p))
        m_h = m_p - 0.5 * (left(m_p) + before)
        alpha = rz / jnp.sum(jnp.where(lane < ITERS, p * m_h, 0.0), axis=1, keepdims=True)
        x = x + alpha * p
        y = y - alpha * h_p
        m_y = m_y - alpha * m_h
        if step + 1 < ITERS:
            rz_next = jnp.sum(jnp.where(lane < ITERS, y * m_y, 0.0), axis=1, keepdims=True)
            beta = rz_next / rz
            p = y + beta * p
            m_p = m_y + beta * m_p
            rz = rz_next
    mean = jnp.sum(jnp.where(lane < ITERS, x * ones, 0.0), axis=1, keepdims=True) / count
    xs = [pick(x, j) for j in range(ITERS)]
    ys = [pick(y, j) for j in range(ITERS + 1)]

    def one(plane, carry):
        weight = scale[plane]
        total = jnp.where(weight > 0.0, -mean, 0.0)
        rest = ys[ITERS] * basis[ITERS, plane]
        for j in range(ITERS):
            value = basis[j, plane]
            total = total + xs[j] * value
            rest = rest + ys[j] * value
        phi[plane] = total
        residual[plane] = weight * rest
        return carry

    lax.fori_loop(0, nz, one, 0)


def body(potential, tissue_mask, layer_index, source):
    extent = tissue_mask.shape
    nz = extent[0]
    labels = tissue_mask.astype(jnp.float32)
    packed = jnp.stack([labels, potential, source], axis=1)
    packed = framed(packed, "gz", 0, 1)
    packed = framed(packed, "gx", 2, 8)
    packed = framed(packed, "gy", 3, 128)
    layers = framed(layer_index, "gz", 0, 1)
    planes = layers.shape[0]
    selector = (layers[:, None] == jnp.arange(LAYERS, dtype=jnp.int32)[None, :]).astype(
        jnp.float32
    )
    tables = jnp.concatenate(
        [
            tensor_table(LAYERS, bulk_long, bulk_trans),
            tensor_table(LAYERS, intra_long, intra_trans),
        ],
        axis=1,
    )
    table = jnp.dot(selector, tables, precision=lax.Precision.HIGHEST)
    size = lax.axis_size("gz")
    link = jnp.ones((planes, 1), jnp.float32)
    if planes == size * nz:
        place = (lax.axis_index("gz") * nz + jnp.arange(planes)) % planes
        link = (place + 1 < planes).astype(jnp.float32)[:, None]
    table = jnp.concatenate([table, link], axis=1)
    frame = (planes,) + packed.shape[2:]
    smem = pl.BlockSpec(memory_space=pltpu.SMEM)
    vmem = pl.BlockSpec(memory_space=pltpu.VMEM)
    compact = frame
    if extent[1] % 8 == 0 and ITERS % 8 == 0 and frame[1] > extent[1] + 2 * ITERS:
        compact = (planes, extent[1] + 2 * ITERS, frame[2])
    sizes = tuple(lax.axis_size(axis) for axis in AXES)
    peers = math.prod(sizes)
    row = pltpu.VMEM((1, 128), jnp.float32)
    gathered = pltpu.VMEM((peers, 1, 128), jnp.float32)
    return tuple(
        pl.pallas_call(
            functools.partial(grid_kernel, extent, sizes),
            out_shape=(jax.ShapeDtypeStruct(extent, jnp.float32),) * 2,
            in_specs=[smem, vmem, vmem, vmem],
            out_specs=(vmem, vmem),
            scratch_shapes=[
                pltpu.VMEM((ITERS + 1,) + extent, jnp.float32),
                pltpu.VMEM(extent, jnp.float32),
                pltpu.VMEM((3 * ITERS, extent[2]), jnp.float32),
                pltpu.VMEM((18,) + compact, jnp.float32),
            ]
            + [pltpu.VMEM(compact, jnp.float32)] * 4
            + [row, gathered, row, gathered]
            + [pltpu.SemaphoreType.DMA((peers,))] * 3,
            compiler_params=pltpu.CompilerParams(
                vmem_limit_bytes=60 * 1024 * 1024, collective_id=0, has_side_effects=True
            ),
        )(table, packed[:, 0], packed[:, 1], packed[:, 2])
    )


def solution(mesh):
    placed = (P("gz", "gx", "gy"), P("gz", "gx", "gy"), P("gz"), P("gz", "gx", "gy"))
    return jax.shard_map(
        body,
        mesh=mesh,
        in_specs=placed,
        out_specs=(P("gz", "gx", "gy"), P("gz", "gx", "gy")),
        check_vma=False,
    )
```

```python
import functools
import math

import jax
import jax.numpy as jnp
from jax import lax
from jax.experimental import pallas as pl
from jax.experimental.pallas import tpu as pltpu
from jax.sharding import PartitionSpec as P

ITERS = 8
DEPTH = ITERS + 1
LAYERS = 16
AXES = ("gx", "gy", "gz")

OFFSETS = [
    (0, 1, 0),
    (0, 0, 1),
    (1, 0, 0),
    (0, 1, 1),
    (0, 1, -1),
    (1, 1, 0),
    (-1, 1, 0),
    (1, 0, 1),
    (-1, 0, 1),
]
bulk_long = 7.99
bulk_trans = 2.55
intra_long = 1.74
intra_trans = 0.19
bath_sigma = 5.0


def tensor_table(layers, longitudinal, transverse):
    depth = jnp.arange(layers, dtype=jnp.float32) / (layers - 1)
    helix = math.pi / 3.0 * (1.0 - 2.0 * depth)
    tilted = 0.35 * jnp.cos(math.pi * depth)
    fiber_x = jnp.cos(tilted) * jnp.cos(helix)
    fiber_y = jnp.cos(tilted) * jnp.sin(helix)
    fiber_z = jnp.sin(tilted)
    spread = longitudinal - transverse
    s_xx = transverse + spread * fiber_x * fiber_x
    s_yy = transverse + spread * fiber_y * fiber_y
    s_zz = transverse + spread * fiber_z * fiber_z
    s_xy = spread * fiber_x * fiber_y
    s_xz = spread * fiber_x * fiber_z
    s_yz = spread * fiber_y * fiber_z
    columns = [
        s_xx - jnp.abs(s_xy) - jnp.abs(s_xz),
        s_yy - jnp.abs(s_xy) - jnp.abs(s_yz),
        s_zz - jnp.abs(s_xz) - jnp.abs(s_yz),
        jnp.maximum(s_xy, 0.0),
        jnp.maximum(-s_xy, 0.0),
        jnp.maximum(s_xz, 0.0),
        jnp.maximum(-s_xz, 0.0),
        jnp.maximum(s_yz, 0.0),
        jnp.maximum(-s_yz, 0.0),
    ]
    return jnp.stack(columns, axis=1)


def shifted(value, axis, hop):
    count = lax.axis_size(axis)
    pairs = [(i + hop, i) for i in range(count) if 0 <= i + hop < count]
    return lax.ppermute(value, axis, pairs)


def framed(value, axis, dim, multiple):
    count, length = lax.axis_size(axis), value.shape[dim]
    if count == 1:
        return value
    if count == 2 and 2 * length <= length + 2 * DEPTH and multiple == 1:
        other = lax.ppermute(value, axis, [(0, 1), (1, 0)])
        return jnp.concatenate([value, other], axis=dim)
    after, before = [], []
    left, hop = DEPTH, 1
    while left > 0:
        width = min(left, length)
        if hop < count:
            after.append(
                shifted(lax.slice_in_dim(value, 0, width, axis=dim), axis, hop)
            )
            before.insert(
                0, shifted(lax.slice_in_dim(value, length - width, length, axis=dim), axis, -hop)
            )
        else:
            shape = list(value.shape)
            shape[dim] = width
            after.append(jnp.zeros(shape, value.dtype))
            before.insert(0, jnp.zeros(shape, value.dtype))
        left, hop = left - width, hop + 1
    gap = -(length + 2 * DEPTH) % multiple
    shape = list(value.shape)
    shape[dim] = gap
    middle = [jnp.zeros(shape, value.dtype)] if gap else []
    return jnp.concatenate([value] + after + middle + before, axis=dim)


def fields_around(ref, here, above, below, rows, lanes):
    def along_x(value, step):
        return pltpu.roll(value, (-step) % rows, 0)

    def along_y(value, step):
        return pltpu.roll(value, (-step) % lanes, 1)

    for dz, plane in ((0, here), (1, above), (-1, below)):
        value = ref[plane]
        if dz:
            yield (dz, 0, 0), value
        for step in (1, -1):
            yield (dz, step, 0), along_x(value, step)
        for step in (1, -1):
            moved = along_y(value, step)
            yield (dz, 0, step), moved
            if dz == 0:
                for other in (1, -1):
                    yield (0, other, step), along_x(moved, other)


SLOT = {}
for _column, _offset in enumerate(OFFSETS):
    SLOT[_offset] = (_column, 2 * _column)
    SLOT[tuple(-o for o in _offset)] = (_column, 2 * _column + 1)


def grid_kernel(extent, sizes, local, table, mask_in, potential_in, source_in, phi, residual,
                basis, scale, dots, weights, spare, first, second, jac,
                own_row, early, final_row, late, sends, early_recv, late_recv, *extra):
    mask, potential, source = mask_in, potential_in, source_in
    if local:
        fields, pack, from_after, from_before, face_send, face_recv = extra
        mask, potential, source = fields.at[0], fields.at[1], fields.at[2]
    planes, rows, lanes = mask.shape
    nz, nx, ny = extent
    held = jac.shape[1]
    keep = nx + ITERS
    peers = math.prod(sizes)
    me = 0
    for axis, size in zip(AXES, sizes):
        me = me * size + lax.axis_index(axis)

    def device(index):
        return (index // (sizes[1] * sizes[2]), index // sizes[2] % sizes[1], index % sizes[2])

    def peer(k):
        return lax.rem(me + k, peers)

    barrier = pltpu.get_barrier_semaphore()

    def greet(k, carry):
        pl.semaphore_signal(
            barrier, inc=1, device_id=device(peer(k)), device_id_type=pl.DeviceIdType.MESH
        )
        return carry

    lax.fori_loop(1, peers, greet, 0)

    def spread(row, gathered, recv):
        def one(k, carry):
            pltpu.make_async_remote_copy(
                src_ref=row, dst_ref=gathered.at[me], send_sem=sends.at[k],
                recv_sem=recv.at[me], device_id=device(peer(k)),
                device_id_type=pl.DeviceIdType.MESH,
            ).start()
            return carry

        lax.fori_loop(1, peers, one, 0)

    def collect(row, gathered, recv):
        def one(k, carry):
            other = peer(k)
            copy = pltpu.make_async_remote_copy(
                src_ref=row, dst_ref=gathered.at[other], send_sem=sends.at[k],
                recv_sem=recv.at[other], device_id=device(other),
                device_id_type=pl.DeviceIdType.MESH,
            )
            copy.wait_recv()
            copy.wait_send()
            return carry

        lax.fori_loop(1, peers, one, 0)
        gathered[me] = row[...]
        return jnp.sum(gathered[...], axis=0)

    lane = lax.broadcasted_iota(jnp.int32, (1, 128), 1)

    def pick(vector, index):
        return jnp.sum(jnp.where(lane == index, vector, 0.0), axis=1, keepdims=True)

    cells = jnp.zeros((1, ny), jnp.float32)
    injected = jnp.zeros((1, ny), jnp.float32)
    for plane in range(nz):
        own_inside = jnp.where(mask_in[plane, 0:nx, 0:ny] > 0.0, 1.0, 0.0)
        cells = cells + jnp.sum(own_inside, axis=0, keepdims=True)
        injected = injected + jnp.sum(
            own_inside * source_in[plane, 0:nx, 0:ny], axis=0, keepdims=True
        )
    cells = jnp.sum(cells, axis=1, keepdims=True)
    injected = jnp.sum(injected, axis=1, keepdims=True)
    own_row[...] = jnp.where(lane == 0, cells, jnp.where(lane == 1, injected, 0.0))

    def neighbours(plane):
        above = jnp.where(plane + 1 == planes, 0, plane + 1)
        below = jnp.where(plane == 0, planes - 1, plane - 1)
        return above, below

    def store(ref, index, value):
        if held == rows:
            ref[index] = value
        else:
            ref[(*index, slice(0, keep))] = value[:keep]
            ref[(*index, slice(keep, held))] = value[rows - held + keep :]

    def setup(plane, carry):
        above, below = neighbours(plane)
        labels = mask[plane]
        tissue = jnp.where(labels == 2.0, 1.0, 0.0)
        bath = jnp.where(labels == 1.0, 1.0, 0.0)
        inside = tissue + bath
        volts = potential[plane]
        total = jnp.zeros((rows, lanes), jnp.float32)
        image = jnp.zeros((rows, lanes), jnp.float32)
        pairs = zip(
            fields_around(mask, plane, above, below, rows, lanes),
            fields_around(potential, plane, above, below, rows, lanes),
        )
        for (offset, label), (_, volt) in pairs:
            column, slot = SLOT[offset]
            beyond = {0: plane, 1: above, -1: below}[offset[0]]
            link = 0.5
            if offset[0] == 1:
                link = 0.5 * table[plane, 18]
            if offset[0] == -1:
                link = 0.5 * table[below, 18]
            their_tissue = jnp.where(label == 2.0, 1.0, 0.0)
            g_here, g_there = table[plane, column] * link, table[beyond, column] * link
            weight = tissue * g_here
            if column < 3:
                their_bath = jnp.where(label == 1.0, 1.0, 0.0)
                sigma = bath_sigma * link
                weight = inside * (
                    jnp.where(label > 0.0, weight + bath * sigma, 0.0)
                    + (their_tissue * g_there + their_bath * sigma)
                )
            else:
                weight = inside * (jnp.where(label > 0.0, weight, 0.0) + their_tissue * g_there)
            store(weights, (slot, plane), weight)
            total = total + weight
            intra = (table[plane, 9 + column] + table[beyond, 9 + column]) * link
            image = image + (tissue * their_tissue * intra) * (volts - volt)
        bounded = jnp.maximum(total, 1.0)
        jacobi = inside / bounded
        store(jac, (plane,), jacobi + jacobi)
        store(spare, (plane,), inside * (1.0 - jacobi * total))
        store(first, (plane,), jacobi * (inside * source[plane] - image))

        @pl.when(plane < nz)
        def _():
            scale[plane] = (inside * bounded)[:nx, :ny]

        return carry

    def faces(axis, moves):
        size = sizes[AXES.index(axis)]
        place = lax.axis_index(axis)
        copies = []
        for slot, step, src, dst in moves:
            copy = pltpu.make_async_remote_copy(
                src_ref=src, dst_ref=dst, send_sem=face_send.at[slot],
                recv_sem=face_recv.at[slot], device_id={axis: place + step},
                device_id_type=pl.DeviceIdType.MESH,
            )
            copies.append((copy, step))
            pl.when((place + step >= 0) & (place + step < size))(copy.start)
        for copy, step in copies:
            pl.when((place - step >= 0) & (place - step < size))(copy.wait_recv)
            pl.when((place + step >= 0) & (place + step < size))(copy.wait_send)

    if local:
        inputs = (mask_in, potential_in, source_in)
        first_x, last_x = lax.axis_index("gx") == 0, lax.axis_index("gx") == sizes[0] - 1
        first_y, last_y = lax.axis_index("gy") == 0, lax.axis_index("gy") == sizes[1] - 1

        @pl.when(last_x)
        def _():
            fields[:, 0:nz, nx : nx + 16, 0:ny] = jnp.zeros((3, nz, 16, ny), jnp.float32)

        @pl.when(first_x)
        def _():
            fields[:, 0:nz, nx + 16 : nx + 32, 0:ny] = jnp.zeros((3, nz, 16, ny), jnp.float32)

        @pl.when(last_y)
        def _():
            from_after[...] = jnp.zeros(from_after.shape, jnp.float32)

        @pl.when(first_y)
        def _():
            from_before[...] = jnp.zeros(from_before.shape, jnp.float32)

        for index, ref in enumerate(inputs):
            fields[index, 0:nz, 0:nx, 0:ny] = ref[...]
        pl.semaphore_wait(barrier, peers - 1)
        spread(own_row, early, early_recv)
        moves = []
        for index, ref in enumerate(inputs):
            to = fields.at[index, pl.ds(0, nz)]
            moves.append(
                (2 * index, 1, ref.at[:, pl.ds(nx - 16, 16)],
                 to.at[:, pl.ds(nx + 16, 16), pl.ds(0, ny)])
            )
            moves.append(
                (2 * index + 1, -1, ref.at[:, pl.ds(0, 16)],
                 to.at[:, pl.ds(nx, 16), pl.ds(0, ny)])
            )
        faces("gx", moves)
        column = lax.broadcasted_iota(jnp.int32, (rows, ny), 1)

        def packing(plane, carry):
            one = pltpu.roll(fields[1, plane, :, 0:ny], 32, 1)
            two = pltpu.roll(fields[2, plane, :, 0:ny], 64, 1)
            value = fields[0, plane, :, 0:ny]
            value = jnp.where((column >= 23) & (column < 41), one, value)
            pack[plane] = jnp.where((column >= 55) & (column < 73), two, value)
            return carry

        lax.fori_loop(0, nz, packing, 0)
        faces("gy", [(6, 1, pack, from_before), (7, -1, pack, from_after)])

        def unpacking(plane, carry):
            for index in range(3):
                after, before = from_after[plane], from_before[plane]
                if index:
                    after = pltpu.roll(after, ny - 32 * index, 1)
                    before = pltpu.roll(before, ny - 32 * index, 1)
                fields[index, plane, :, ny : 2 * ny] = jnp.where(
                    column < DEPTH, after, jnp.where(column >= ny - DEPTH, before, 0.0)
                )
            return carry

        lax.fori_loop(0, nz, unpacking, 0)
        side = lax.axis_index("gz")
        swap = pltpu.make_async_remote_copy(
            src_ref=fields.at[:, pl.ds(0, nz)], dst_ref=fields.at[:, pl.ds(nz, nz)],
            send_sem=face_send.at[8], recv_sem=face_recv.at[8],
            device_id={"gz": 1 - side}, device_id_type=pl.DeviceIdType.MESH,
        )
        swap.start()
        swap.wait()
        lax.fori_loop(0, planes, setup, 0)
    else:
        lax.fori_loop(0, planes // 2, setup, 0)
        pl.semaphore_wait(barrier, peers - 1)
        spread(own_row, early, early_recv)
        lax.fori_loop(planes // 2, planes, setup, 0)
    totals = collect(own_row, early, early_recv)
    count = pick(totals, 0)
    mean_rhs = pick(totals, 1) / count

    def centre(plane, carry):
        first[plane] = first[plane] - 0.5 * jac[plane] * mean_rhs
        return carry

    lax.fori_loop(0, planes, centre, 0)

    def record(step, now, before):
        rowsum = jnp.zeros((1, ny), jnp.float32)
        square, cross, plain = rowsum, rowsum, rowsum
        for plane in range(nz):
            value = now[plane, 0:nx, 0:ny]
            basis[step, plane] = value
            weighted = value * scale[plane]
            square = square + jnp.sum(weighted * value, axis=0, keepdims=True)
            if step:
                past = basis[step - 1, plane]
                cross = cross + jnp.sum(weighted * past, axis=0, keepdims=True)
            plain = plain + jnp.sum(value, axis=0, keepdims=True)
        if step < ITERS:
            dots[pl.ds(2 * step, 1)] = square
            dots[pl.ds(2 * ITERS + step, 1)] = plain
        if step:
            dots[pl.ds(2 * step - 1, 1)] = cross

    record(0, first, None)

    def apply(now, old, step):
        reach = ITERS - step
        if planes == nz:
            begin, span = 0, nz
        elif planes == sizes[2] * nz:
            begin = planes - lax.axis_index("gz") * reach
            span = min(planes, nz + reach)
        else:
            begin, span = planes - reach, nz + 2 * reach

        def one(index, carry):
            plane = lax.rem(begin + index, planes)
            above, below = neighbours(plane)
            total = jnp.zeros((held, lanes), jnp.float32)
            for offset, value in fields_around(now, plane, above, below, held, lanes):
                total = total + weights[SLOT[offset][1], plane] * value
            if step == 1:
                old[plane] = 0.5 * jac[plane] * total + spare[plane] * now[plane]
            else:
                old[plane] = (
                    jac[plane] * total + 2.0 * spare[plane] * now[plane] - old[plane]
                )
            return carry

        lax.fori_loop(0, span, one, 0)

    now, old = first, second
    for step in range(1, ITERS + 1):
        apply(now, old, step)
        now, old = old, now
        record(step, now, old)

    partial = jnp.sum(dots[...], axis=1, keepdims=True)
    diagonal = lax.broadcasted_iota(jnp.int32, (3 * ITERS, 128), 0) == lax.broadcasted_iota(
        jnp.int32, (3 * ITERS, 128), 1
    )
    final_row[...] = jnp.sum(jnp.where(diagonal, partial, 0.0), axis=0, keepdims=True)
    spread(final_row, late, late_recv)
    sums = collect(final_row, late, late_recv)

    def left(vector):
        return pltpu.roll(vector, 127, 1)

    def right(vector):
        return pltpu.roll(vector, 1, 1)

    mu0, mu1 = pick(sums, 0), pick(sums, 1)
    mu = jnp.where(lane < 2, sums, 2.0 * sums - jnp.where(lane % 2 == 0, mu0, mu1))
    mu = jnp.where(lane < 2 * ITERS, mu, 0.0)
    ones = pltpu.roll(sums, 128 - 2 * ITERS, 1)
    y = jnp.where(lane == 0, 1.0, 0.0)
    p = y
    m_y, m_p = mu, mu
    x = jnp.zeros((1, 128), jnp.float32)
    rz = mu0
    for step in range(ITERS):
        h_p = p - 0.5 * (left(p) + jnp.where(lane == 1, 2.0, 1.0) * right(p))
        h_p = jnp.where(lane <= ITERS, h_p, 0.0)
        before = jnp.where(lane == 0, left(m_p), right(m_p))
        m_h = m_p - 0.5 * (left(m_p) + before)
        alpha = rz / jnp.sum(jnp.where(lane < ITERS, p * m_h, 0.0), axis=1, keepdims=True)
        x = x + alpha * p
        y = y - alpha * h_p
        m_y = m_y - alpha * m_h
        if step + 1 < ITERS:
            rz_next = jnp.sum(jnp.where(lane < ITERS, y * m_y, 0.0), axis=1, keepdims=True)
            beta = rz_next / rz
            p = y + beta * p
            m_p = m_y + beta * m_p
            rz = rz_next
    mean = jnp.sum(jnp.where(lane < ITERS, x * ones, 0.0), axis=1, keepdims=True) / count
    xs = [pick(x, j) for j in range(ITERS)]
    ys = [pick(y, j) for j in range(ITERS + 1)]

    def one(plane, carry):
        weight = scale[plane]
        total = jnp.where(weight > 0.0, -mean, 0.0)
        rest = ys[ITERS] * basis[ITERS, plane]
        for j in range(ITERS):
            value = basis[j, plane]
            total = total + xs[j] * value
            rest = rest + ys[j] * value
        phi[plane] = total
        residual[plane] = weight * rest
        return carry

    lax.fori_loop(0, nz, one, 0)


def body(potential, tissue_mask, layer_index, source):
    extent = tissue_mask.shape
    nz = extent[0]
    labels = tissue_mask.astype(jnp.float32)
    sizes = tuple(lax.axis_size(axis) for axis in AXES)
    local = (
        sizes[2] == 2 and nz <= DEPTH and extent[1] % 8 == 0 and extent[1] >= 16
        and extent[2] == 128
    )
    if local:
        operands = (labels, potential, source)
        frame = (2 * nz, extent[1] + 32, 2 * extent[2])
    else:
        packed = jnp.stack([labels, potential, source], axis=1)
        packed = framed(packed, "gz", 0, 1)
        packed = framed(packed, "gx", 2, 8)
        packed = framed(packed, "gy", 3, 128)
        operands = (packed[:, 0], packed[:, 1], packed[:, 2])
        frame = operands[0].shape
    layers = framed(layer_index, "gz", 0, 1)
    planes = layers.shape[0]
    selector = (layers[:, None] == jnp.arange(LAYERS, dtype=jnp.int32)[None, :]).astype(
        jnp.float32
    )
    tables = jnp.concatenate(
        [
            tensor_table(LAYERS, bulk_long, bulk_trans),
            tensor_table(LAYERS, intra_long, intra_trans),
        ],
        axis=1,
    )
    table = jnp.dot(selector, tables, precision=lax.Precision.HIGHEST)
    size = lax.axis_size("gz")
    link = jnp.ones((planes, 1), jnp.float32)
    if planes == size * nz:
        place = (lax.axis_index("gz") * nz + jnp.arange(planes)) % planes
        link = (place + 1 < planes).astype(jnp.float32)[:, None]
    table = jnp.concatenate([table, link], axis=1)
    smem = pl.BlockSpec(memory_space=pltpu.SMEM)
    vmem = pl.BlockSpec(memory_space=pltpu.VMEM)
    compact = frame
    if extent[1] % 8 == 0 and ITERS % 8 == 0 and frame[1] > extent[1] + 2 * ITERS:
        compact = (planes, extent[1] + 2 * ITERS, frame[2])
    strip = pltpu.VMEM((nz,) + (frame[1], extent[2]), jnp.float32)
    extra = []
    if local:
        extra = [pltpu.VMEM((3,) + frame, jnp.float32), strip, strip, strip]
        extra += [pltpu.SemaphoreType.DMA((9,))] * 2
    peers = math.prod(sizes)
    row = pltpu.VMEM((1, 128), jnp.float32)
    gathered = pltpu.VMEM((peers, 1, 128), jnp.float32)
    return tuple(
        pl.pallas_call(
            functools.partial(grid_kernel, extent, sizes, local),
            out_shape=(jax.ShapeDtypeStruct(extent, jnp.float32),) * 2,
            in_specs=[smem, vmem, vmem, vmem],
            out_specs=(vmem, vmem),
            scratch_shapes=[
                pltpu.VMEM((ITERS + 1,) + extent, jnp.float32),
                pltpu.VMEM(extent, jnp.float32),
                pltpu.VMEM((3 * ITERS, extent[2]), jnp.float32),
                pltpu.VMEM((18,) + compact, jnp.float32),
            ]
            + [pltpu.VMEM(compact, jnp.float32)] * 4
            + [row, gathered, row, gathered]
            + [pltpu.SemaphoreType.DMA((peers,))] * 3
            + extra,
            compiler_params=pltpu.CompilerParams(
                vmem_limit_bytes=60 * 1024 * 1024, collective_id=0, has_side_effects=True
            ),
        )(table, *operands)
    )


def solution(mesh):
    placed = (P("gz", "gx", "gy"), P("gz", "gx", "gy"), P("gz"), P("gz", "gx", "gy"))
    return jax.shard_map(
        body,
        mesh=mesh,
        in_specs=placed,
        out_specs=(P("gz", "gx", "gy"), P("gz", "gx", "gy")),
        check_vma=False,
    )
```
